32 devices in a mesh: img: 2 (over x), ga: 4 (over y, core), band: 4 (over z).
Axes of the slice: x: 2, y: 2, z: 4, core: 2. Of those that a mesh axis runs over, the one named last changes fastest.
Arguments:
- orbitals: bfloat16 [1536, 12288], P(('img', 'band'), 'ga'), parts along dimension 0, as said below
- kernel: float32 [12288], P('ga'), may hold values from 0.3 to 3
- block_vectors: bfloat16 [512, 12288], P(('img', 'band'), 'ga'), parts along dimension 0
Outputs:
- ace_vectors: bfloat16 [1536, 12288], P(('img', 'band'), 'ga'), parts along dimension 0
- exchange_block: bfloat16 [512, 12288], P(('img', 'band'), 'ga'), parts along dimension 0
The draws below stay inside these ranges and needn't reach their ends.
There are 2 independent parts, one for each index of `img`. The reference program is written for one: setup_inputs(seed, part) draws one part's arguments, and reference() takes and returns one part's arrays. A program takes and returns all parts, laid end to end along the dimension named above; an argument that names none is the same for every part. Nothing has to cross between parts.
Inputs may be any that keep to these rules, and one draw needn't show every extreme that they name: `orbitals`: the bands of one image are linearly independent, and the block lies largely in their span.
All inputs are finite; a program needn't handle non-finite values.
Results may differ from the reference program's by a relative error of at most 0.02.
Values may be sent and summed in bfloat16 or wider, within the bound.
A program may use at most 64 MiB of HBM per device.

```python
import math
import jax
import jax.numpy as jnp
from jax import lax

NB = 768
NBLK = 256
NG = 12288


def orbital_pair(key):
    independent = jax.random.normal(jax.random.fold_in(key, 11), (NB, NG), jnp.float32)
    mixing = jax.random.normal(jax.random.fold_in(key, 12), (NB, NB), jnp.float32) * (0.4 / math.sqrt(NB))
    orbital_rows = independent + jnp.dot(mixing, independent, precision=lax.Precision.HIGHEST)
    mixture = jax.random.normal(jax.random.fold_in(key, 13), (NBLK, NB), jnp.float32) / math.sqrt(NB)
    residue = jax.random.normal(jax.random.fold_in(key, 14), (NBLK, NG), jnp.float32)
    block_rows = jnp.dot(mixture, orbital_rows, precision=lax.Precision.HIGHEST) + 0.5 * residue
    return (orbital_rows, block_rows)


def draw_orbitals(key, part):
    return orbital_pair(key)[0].astype(jnp.bfloat16)


def draw_block_vectors(key, part):
    return orbital_pair(key)[1].astype(jnp.bfloat16)


def steps_of(rng, extent, pieces, least, high):
    gain, own = 1.0, jax.random.fold_in(rng, 6)
    for position, blocks in pieces:
        heights = jnp.exp(jax.random.uniform(jax.random.fold_in(own, position), (blocks,), jnp.float32, least / len(pieces), high / len(pieces)))
        gain = gain * jnp.repeat(heights, extent[position] // blocks).reshape([-1 if axis == position else 1 for axis in range(len(extent))])
    return gain


def setup_inputs(seed: int = 0, part: int = 0) -> dict:
    arg_keys = jax.random.split(jax.random.key(seed), 4)
    part_keys = jax.random.split(jax.random.fold_in(arg_keys[3], part), 4)
    orbitals = draw_orbitals(jax.random.fold_in(jax.random.fold_in(arg_keys[3], part), 71), part)
    kernel = jnp.clip(jnp.exp(math.log(3.0) - 2.3025851 * jax.random.uniform(arg_keys[1], (NG,), jnp.float32) ** steps_of(arg_keys[1], (NG,), ((0, 4),), -0.2, 0.2)), 0.3, 3.0)
    block_vectors = draw_block_vectors(jax.random.fold_in(jax.random.fold_in(arg_keys[3], part), 71), part)
    return {"orbitals": orbitals, "kernel": kernel, "block_vectors": block_vectors}


def reference(orbitals, kernel, block_vectors):
    weighted = (-(orbitals.astype(jnp.float32) * kernel[None, :])).astype(jnp.bfloat16)
    margin = -lax.dot_general(orbitals.astype(jnp.float32), weighted.astype(jnp.float32), (((1,), (1,)), ((), ())), preferred_element_type=jnp.float32) / NG
    factor = jnp.linalg.cholesky(margin)
    projector = lax.linalg.triangular_solve(factor, weighted.astype(jnp.float32), left_side=True, lower=True)
    coupling = jnp.dot(projector, block_vectors.astype(jnp.float32).T, precision=lax.Precision.HIGHEST) / NG
    applied = -lax.dot_general(coupling, projector, (((0,), (0,)), ((), ())), precision=lax.Precision.HIGHEST)
    return (projector.astype(jnp.bfloat16), applied.astype(jnp.bfloat16))
```

```python
import functools

import jax
import jax.numpy as jnp
from jax import lax
from jax.experimental import pallas as pl
from jax.experimental.pallas import tpu as pltpu
from jax.sharding import PartitionSpec as P

MESH = pl.DeviceIdType.MESH
F32 = jnp.float32
BF16 = jnp.bfloat16
TILE = 128


def send(src, dst, send_sem, recv_sem, where):
    copy = pltpu.make_async_remote_copy(
        src_ref=src, dst_ref=dst, send_sem=send_sem, recv_sem=recv_sem,
        device_id=where, device_id_type=MESH,
    )
    copy.start()
    return copy


def greet(places):
    barrier = pltpu.get_barrier_semaphore()
    for place in places:
        pl.semaphore_signal(barrier, inc=1, device_id=place, device_id_type=MESH)
    pl.semaphore_wait(barrier, len(places))


def dot(a, b, dims):
    return lax.dot_general(a, b, (dims, ((), ())), preferred_element_type=F32)


def margin_kernel(bands, groups, orb, kern, blk, m_out, s_out, w_out,
                  full, part32, part16, rx_core, acc, out_z, rx_z, out_y, rx_y, allg,
                  a_s, a_r, b_s, b_r, loc, c_s, c_r, z_s, z_r, y_s, y_r, g_s, g_r, f_s, f_r):
    me = lax.axis_index("band")
    ga = lax.axis_index("ga")
    own, bown = orb.shape[0], blk.shape[0]
    cols = orb.shape[1] // bands
    n = own * bands
    half = full.shape[0] // 2
    total = orb.shape[1] * groups
    core = lax.rem(ga, 2)
    partner = {"ga": ga + 1 - 2 * core}
    peer = [lax.rem(me + d, bands) for d in range(bands)]
    order = sorted(range(1, bands), key=lambda d: -min(d, bands - d))
    bits = []
    stride = 2
    while stride < groups:
        bits.append({"ga": ga + stride * (1 - 2 * lax.rem(ga // stride, 2))})
        stride *= 2
    greet([{"band": peer[d]} for d in range(1, bands)] + [partner] + bits)

    def chunk(d):
        return pl.ds(pl.multiple_of(peer[d] * cols, TILE), cols)

    mine = pl.ds(pl.multiple_of(me * own, 16), own)
    mine_b = pl.ds(pl.multiple_of(n + me * bown, 16), bown)
    local_a = pltpu.make_async_copy(orb.at[:, chunk(0)], full.at[mine], loc.at[0])
    local_a.start()
    local_b = pltpu.make_async_copy(blk.at[:, chunk(0)], full.at[mine_b], loc.at[1])
    local_b.start()
    copies_a = [send(orb.at[:, chunk(d)], full.at[mine], a_s.at[d], a_r.at[d], {"band": peer[d]})
                for d in order]
    copies_b = [send(blk.at[:, chunk(d)], full.at[mine_b], b_s.at[d], b_r.at[d], {"band": peer[d]})
                for d in order]
    local_a.wait()
    local_b.wait()
    for copy in copies_a:
        copy.wait()
    w_out[...] = (-(full[0:n, :].astype(F32) * kern[:, chunk(0)])).astype(BF16)
    for copy in copies_b:
        copy.wait()
    for h in range(2):
        product = dot(w_out[...], full[h * half:(h + 1) * half, :], ((1,), (1,)))
        part32[h] = product
        part16[h] = product.astype(BF16)
    send(part16.at[1 - core], rx_core, c_s, c_r, partner).wait()
    acc[...] = part32[core] + rx_core[...].astype(F32)
    out_z[...] = acc[...].astype(BF16)
    copies = [send(out_z.at[pl.ds(pl.multiple_of(peer[d] * own, 16), own)], rx_z.at[d],
                   z_s.at[d], z_r.at[d], {"band": peer[d]}) for d in order]
    for copy in copies:
        copy.wait()
    total_rows = acc[mine, :]
    for d in range(1, bands):
        total_rows = total_rows + rx_z[d].astype(F32)
    for i, place in enumerate(bits):
        out_y[i] = total_rows.astype(BF16)
        send(out_y.at[i], rx_y.at[i], y_s.at[i], y_r.at[i], place).wait()
        total_rows = out_y[i].astype(F32) + rx_y[i].astype(F32)
    allg[core, mine, :] = total_rows.astype(BF16)
    block = allg.at[core, mine]
    copies = {d: send(block, block, g_s.at[d], g_r.at[d], {"band": peer[d]}) for d in order}
    forwards = [send(block, block, f_s.at[0], f_r.at[0], partner)]
    for d in sorted(range(1, bands), key=lambda d: min(d, bands - d)):
        copies[d].wait()
        source = lax.rem(me + bands - d, bands)
        there = allg.at[core, pl.ds(pl.multiple_of(source * own, 16), own)]
        forwards.append(send(there, there, f_s.at[d], f_r.at[d], partner))
    for copy in forwards:
        copy.wait()
    scale = 1.0 / total
    m_out[:, 0:half] = allg[0].astype(F32) * -scale
    m_out[:, half:n] = allg[1, :, 0:n - half].astype(F32) * -scale
    s_out[...] = (allg[1, :, n - half:].astype(F32) * scale).astype(BF16)


def split(a):
    high = a.astype(BF16)
    return high, (a - high.astype(F32)).astype(BF16)


def product3(a, b, dims):
    (ah, al), (bh, bl) = split(a), split(b)
    return dot(ah, bh, dims) + (dot(ah, bl, dims) + dot(al, bh, dims))


def identity(rows):
    shape = (rows, rows)
    return (lax.broadcasted_iota(jnp.int32, shape, 0)
            == lax.broadcasted_iota(jnp.int32, shape, 1)).astype(F32)


def factor_tile(d_ref, t_ref):
    G = 8
    sub = lax.broadcasted_iota(jnp.int32, (G, TILE), 0)

    def spread(row):
        return jnp.broadcast_to(row, (G, TILE))

    def step(g, carry):
        start = pl.multiple_of(g * G, G)
        left = d_ref[pl.ds(start, G), 0:TILE]
        right = d_ref[pl.ds(start, G), TILE:2 * TILE]
        turned = pltpu.roll(left, lax.rem(TILE - start, TILE), 1)
        columns = [jnp.broadcast_to(turned[:, c:c + 1], (G, TILE)) for c in range(G)]
        d = [[spread(columns[c][i:i + 1, :]) for c in range(i + 1)] for i in range(G)]
        u, v = [], []
        u_all = v_all = jnp.zeros((G, TILE), F32)
        for j in range(G):
            r = lax.rsqrt(d[j][j])
            for i in range(j + 1, G):
                d[i][j] = d[i][j] * r
            for i in range(j + 1, G):
                for c in range(j + 1, i + 1):
                    d[i][c] = d[i][c] - d[i][j] * d[c][j]
            a, b = spread(left[j:j + 1, :]), spread(right[j:j + 1, :])
            for t in range(j):
                a = a - d[j][t] * u[t]
                b = b - d[j][t] * v[t]
            u.append(a * r)
            v.append(b * r)
            u_all = jnp.where(sub == j, u[j], u_all)
            v_all = jnp.where(sub == j, v[j], v_all)
        t_ref[pl.ds(start, G), :] = v_all
        both = jnp.concatenate([u_all, v_all], axis=1)
        high = both.astype(BF16).astype(F32)
        low = both - high
        lhs = jnp.concatenate([high[:, :TILE], high[:, :TILE], low[:, :TILE], low[:, :TILE]], axis=0)
        rhs = jnp.concatenate([high, low, high, low], axis=0)
        d_ref[...] -= dot(lhs.astype(BF16), rhs.astype(BF16), ((0,), (0,)))
        return carry

    lax.fori_loop(0, TILE // G, step, 0)


def factor_kernel(m_ref, x_ref, a, rest, d_ref, t_ref):
    n = m_ref.shape[0]
    a[...] = m_ref[...]
    rest[...] = identity(n)
    x_ref[...] = jnp.zeros_like(x_ref)
    for s in range(0, n, TILE):
        e = s + TILE
        d_ref[:, 0:TILE] = a[s:e, s:e]
        d_ref[:, TILE:] = identity(TILE)
        factor_tile(d_ref, t_ref)
        tile = t_ref[...]
        rows = product3(tile, rest[s:e, 0:e], ((1,), (0,)))
        x_ref[s:e, 0:e] = rows.astype(BF16)
        if e < n:
            panel = product3(a[e:, s:e], tile, ((1,), (1,)))
            a[e:, e:] -= product3(panel, panel, ((1,), (1,)))
            rest[e:, 0:e] -= product3(panel, rows, ((1,), (0,)))


def apply_kernel(bands, x, s, w, ace, exch, proj, applied, p_s, p_r, e_s, e_r, loc):
    me = lax.axis_index("band")
    own, bown = ace.shape[0], exch.shape[0]
    cols = w.shape[1]
    peer = [lax.rem(me + d, bands) for d in range(bands)]
    order = sorted(range(1, bands), key=lambda d: -min(d, bands - d))
    greet([{"band": peer[d]} for d in range(1, bands)])
    here = pl.ds(pl.multiple_of(me * cols, TILE), cols)
    copies = []
    for d in order + [0]:
        rows = pl.ds(pl.multiple_of(peer[d] * own, 16), own)
        proj[rows, :] = dot(x[rows, :], w[...], ((1,), (0,))).astype(BF16)
        if d:
            copies.append(send(proj.at[rows], ace.at[:, here], p_s.at[d], p_r.at[d], {"band": peer[d]}))
        else:
            copies.append(pltpu.make_async_copy(proj.at[rows], ace.at[:, here], loc.at[0]))
            copies[-1].start()
    coupling = dot(x[...], s[...], ((1,), (0,))).astype(BF16)
    applied[...] = (-dot(coupling, proj[...], ((0,), (0,)))).astype(BF16)
    for d in order + [0]:
        rows = pl.ds(pl.multiple_of(peer[d] * bown, 16), bown)
        if d:
            copies.append(send(applied.at[rows], exch.at[:, here], e_s.at[d], e_r.at[d], {"band": peer[d]}))
        else:
            copies.append(pltpu.make_async_copy(applied.at[rows], exch.at[:, here], loc.at[1]))
            copies[-1].start()
    for copy in copies:
        copy.wait()


def shards(orbitals, kernel, block_vectors):
    groups, bands = lax.axis_size("ga"), lax.axis_size("band")
    own, width = orbitals.shape
    bown = block_vectors.shape[0]
    cols = width // bands
    n, nblk = own * bands, bown * bands
    half = (n + nblk) // 2
    levels = max(groups.bit_length() - 2, 1)
    vmem, hbm = pl.BlockSpec(memory_space=pltpu.VMEM), pl.BlockSpec(memory_space=pl.ANY)
    dma = pltpu.SemaphoreType.DMA
    many = dma((bands,))
    margin, s, weighted = pl.pallas_call(
        functools.partial(margin_kernel, bands, groups),
        name="margin",
        out_shape=(
            jax.ShapeDtypeStruct((n, n), F32),
            jax.ShapeDtypeStruct((n, nblk), BF16),
            jax.ShapeDtypeStruct((n, cols), BF16),
        ),
        in_specs=[hbm, vmem, hbm],
        out_specs=(vmem, vmem, vmem),
        scratch_shapes=[
            pltpu.VMEM((n + nblk, cols), BF16),
            pltpu.VMEM((2, n, half), F32),
            pltpu.VMEM((2, n, half), BF16),
            pltpu.VMEM((n, half), BF16),
            pltpu.VMEM((n, half), F32),
            pltpu.VMEM((n, half), BF16),
            pltpu.VMEM((bands, own, half), BF16),
            pltpu.VMEM((levels, own, half), BF16),
            pltpu.VMEM((levels, own, half), BF16),
            pltpu.VMEM((2, n, half), BF16),
            many, many, many, many, dma((2,)), dma, dma, many, many,
            dma((levels,)), dma((levels,)), many, many, many, many,
        ],
        compiler_params=pltpu.CompilerParams(
            collective_id=0, has_side_effects=True, vmem_limit_bytes=48 * 2**20),
    )(orbitals, kernel.reshape(1, width), block_vectors)
    inverse = pl.pallas_call(
        factor_kernel,
        name="factor",
        out_shape=jax.ShapeDtypeStruct((n, n), BF16),
        in_specs=[vmem],
        out_specs=vmem,
        scratch_shapes=[
            pltpu.VMEM((n, n), F32),
            pltpu.VMEM((n, n), F32),
            pltpu.VMEM((TILE, 2 * TILE), F32),
            pltpu.VMEM((TILE, TILE), F32),
        ],
        compiler_params=pltpu.CompilerParams(vmem_limit_bytes=48 * 2**20),
    )(margin)
    return pl.pallas_call(
        functools.partial(apply_kernel, bands),
        name="apply",
        out_shape=(
            jax.ShapeDtypeStruct((own, width), BF16),
            jax.ShapeDtypeStruct((bown, width), BF16),
        ),
        in_specs=[vmem, vmem, vmem],
        out_specs=(hbm, hbm),
        scratch_shapes=[
            pltpu.VMEM((n, cols), BF16),
            pltpu.VMEM((nblk, cols), BF16),
            many, many, many, many, dma((2,)),
        ],
        compiler_params=pltpu.CompilerParams(
            collective_id=1, has_side_effects=True, vmem_limit_bytes=48 * 2**20),
    )(inverse, s, weighted)


def solution(mesh):
    placed = (P(("img", "band"), "ga"), P("ga"), P(("img", "band"), "ga"))
    return jax.shard_map(
        shards,
        mesh=mesh,
        in_specs=placed,
        out_specs=(P(("img", "band"), "ga"), P(("img", "band"), "ga")),
        check_vma=False,
    )
```

```python
import functools

import jax
import jax.numpy as jnp
from jax import lax
from jax.experimental import pallas as pl
from jax.experimental.pallas import tpu as pltpu
from jax.sharding import PartitionSpec as P

MESH = pl.DeviceIdType.MESH
F32 = jnp.float32
BF16 = jnp.bfloat16
TILE = 128


def send(src, dst, send_sem, recv_sem, where):
    copy = pltpu.make_async_remote_copy(
        src_ref=src, dst_ref=dst, send_sem=send_sem, recv_sem=recv_sem,
        device_id=where, device_id_type=MESH,
    )
    copy.start()
    return copy


def greet(places):
    barrier = pltpu.get_barrier_semaphore()
    for place in places:
        pl.semaphore_signal(barrier, inc=1, device_id=place, device_id_type=MESH)
    pl.semaphore_wait(barrier, len(places))


def dot(a, b, dims):
    return lax.dot_general(a, b, (dims, ((), ())), preferred_element_type=F32)


class Place:
    def __init__(self, bands, groups):
        self.bands = bands
        self.me = lax.axis_index("band")
        ga = lax.axis_index("ga")
        self.core = lax.rem(ga, 2)
        self.row = lax.rem(ga // 2, 2)
        self.partner = {"ga": ga + 1 - 2 * self.core}
        self.across = {"ga": ga + 2 - 4 * self.row}
        self.peer = [lax.rem(self.me + d, bands) for d in range(bands)]
        self.far = sorted(range(1, bands), key=lambda d: -min(d, bands - d))
        self.near = self.far[::-1]
        self.bits = []
        stride = 4
        while stride < groups:
            self.bits.append({"ga": ga + stride * (1 - 2 * lax.rem(ga // stride, 2))})
            stride *= 2

    def band(self, d):
        return {"band": self.peer[d]}

    def everyone(self):
        return [self.band(d) for d in range(1, self.bands)] + [self.partner, self.across] + self.bits


def span(index, size, offset=0):
    return pl.ds(pl.multiple_of(offset + index * size, 16), size)


def reduce_scratch(rows, bands, levels):
    h1, h2 = rows // 2, rows // 4
    h3 = h2 // bands
    dma = pltpu.SemaphoreType.DMA
    shapes = [
        ((rows, TILE), F32), ((rows, TILE), BF16), ((h1, TILE), BF16),
        ((h1, TILE), F32), ((h1, TILE), BF16), ((h2, TILE), BF16),
        ((h2, TILE), F32), ((h2, TILE), BF16), ((bands, h3, TILE), BF16),
        ((levels, h3, TILE), BF16), ((levels, h3, TILE), BF16), ((rows, TILE), BF16),
    ]
    return [pltpu.VMEM(*shape) for shape in shapes] + [
        dma((4,)), dma((bands,)), dma((bands,)), dma((levels,)), dma((levels,)),
        dma((bands,)), dma((bands,)), dma((bands,)), dma((bands,)),
        dma((2 * bands,)), dma((2 * bands,)),
    ]


def reduce_stages(at, scratch):
    (p32, p16, rx1, a32, a16, rx2, b32, b16, rx3, out_x, rx_x, allg,
     one, z_s, z_r, x_s, x_r, g_s, g_r, y_s, y_r, f_s, f_r) = scratch
    h1, h2 = rx1.shape[0], rx2.shape[0]
    h3 = h2 // at.bands
    copy = send(p16.at[span(1 - at.core, h1)], rx1, one.at[0], one.at[1], at.partner)
    yield
    copy.wait()
    a32[...] = p32[span(at.core, h1), :] + rx1[...].astype(F32)
    a16[...] = a32[...].astype(BF16)
    copy = send(a16.at[span(1 - at.row, h2)], rx2, one.at[2], one.at[3], at.across)
    yield
    copy.wait()
    b32[...] = a32[span(at.row, h2), :] + rx2[...].astype(F32)
    b16[...] = b32[...].astype(BF16)
    copies = [send(b16.at[span(at.peer[d], h3)], rx3.at[d], z_s.at[d], z_r.at[d], at.band(d))
              for d in at.far]
    yield
    for copy in copies:
        copy.wait()
    total = b32[span(at.me, h3), :]
    for d in range(1, at.bands):
        total = total + rx3[d].astype(F32)
    for i, place in enumerate(at.bits):
        out_x[i] = total.astype(BF16)
        send(out_x.at[i], rx_x.at[i], x_s.at[i], x_r.at[i], place).wait()
        total = out_x[i].astype(F32) + rx_x[i].astype(F32)

    def piece(d, row):
        source = lax.rem(at.me + at.bands - d, at.bands)
        return allg.at[span(source, h3, at.core * h1 + row * h2)]

    allg[span(at.me, h3, at.core * h1 + at.row * h2), :] = total.astype(BF16)
    own = piece(0, at.row)
    gathers = {d: send(own, own, g_s.at[d], g_r.at[d], at.band(d)) for d in at.far}
    sides = {0: send(own, own, y_s.at[0], y_r.at[0], at.across)}
    lasts = [send(own, own, f_s.at[0], f_r.at[0], at.partner)]
    yield
    for d in at.near:
        gathers[d].wait()
        there = piece(d, at.row)
        sides[d] = send(there, there, y_s.at[d], y_r.at[d], at.across)
        lasts.append(send(there, there, f_s.at[d], f_r.at[d], at.partner))
    yield
    for d in [0] + at.near:
        sides[d].wait()
        there = piece(d, 1 - at.row)
        e = at.bands + d
        lasts.append(send(there, there, f_s.at[e], f_r.at[e], at.partner))
    yield
    for copy in lasts:
        copy.wait()


def margin_kernel(bands, groups, orb, kern, m_out, w_out, full, loc, a_s, a_r, *scratch):
    at = Place(bands, groups)
    own = orb.shape[0]
    cols = orb.shape[1] // bands
    n = own * bands
    greet(at.everyone())

    def chunk(d):
        return pl.ds(pl.multiple_of(at.peer[d] * cols, TILE), cols)

    mine = full.at[span(at.me, own)]
    local = pltpu.make_async_copy(orb.at[:, chunk(0)], mine, loc.at[0])
    local.start()
    copies = [send(orb.at[:, chunk(d)], mine, a_s.at[d], a_r.at[d], at.band(d)) for d in at.far]
    local.wait()
    for copy in copies:
        copy.wait()
    w_out[...] = (-(full[...].astype(F32) * kern[:, chunk(0)])).astype(BF16)
    p32, p16, allg = scratch[0], scratch[1], scratch[11]
    row = 0
    for s in range(0, n, TILE):
        e = s + TILE
        product = dot(w_out[s:e, :], full[0:e, :], ((1,), (1,)))
        for c in range(0, e, TILE):
            p32[row:row + TILE, :] = product[:, c:c + TILE]
            p16[row:row + TILE, :] = product[:, c:c + TILE].astype(BF16)
            row += TILE
    if row < p32.shape[0]:
        p32[row:, :] = jnp.zeros((p32.shape[0] - row, TILE), F32)
        p16[row:, :] = jnp.zeros((p32.shape[0] - row, TILE), BF16)
    for _ in reduce_stages(at, scratch):
        pass
    m_out[...] = allg[...]


def split(a):
    high = a.astype(BF16)
    return high, (a - high.astype(F32)).astype(BF16)


def product3(a, b, dims):
    (ah, al), (bh, bl) = split(a), split(b)
    return dot(ah, bh, dims) + (dot(ah, bl, dims) + dot(al, bh, dims))


def identity(rows):
    shape = (rows, rows)
    return (lax.broadcasted_iota(jnp.int32, shape, 0)
            == lax.broadcasted_iota(jnp.int32, shape, 1)).astype(F32)


def factor_tile(d_ref, t_ref):
    G = 8
    sub = lax.broadcasted_iota(jnp.int32, (G, TILE), 0)

    def spread(row):
        return jnp.broadcast_to(row, (G, TILE))

    def step(g, carry):
        start = pl.multiple_of(g * G, G)
        left = d_ref[pl.ds(start, G), 0:TILE]
        right = d_ref[pl.ds(start, G), TILE:2 * TILE]
        turned = pltpu.roll(left, lax.rem(TILE - start, TILE), 1)
        columns = [jnp.broadcast_to(turned[:, c:c + 1], (G, TILE)) for c in range(G)]
        d = [[spread(columns[c][i:i + 1, :]) for c in range(i + 1)] for i in range(G)]
        u, v = [], []
        u_all = v_all = jnp.zeros((G, TILE), F32)
        for j in range(G):
            r = lax.rsqrt(d[j][j])
            for i in range(j + 1, G):
                d[i][j] = d[i][j] * r
            for i in range(j + 1, G):
                for c in range(j + 1, i + 1):
                    d[i][c] = d[i][c] - d[i][j] * d[c][j]
            a, b = spread(left[j:j + 1, :]), spread(right[j:j + 1, :])
            for t in range(j):
                a = a - d[j][t] * u[t]
                b = b - d[j][t] * v[t]
            u.append(a * r)
            v.append(b * r)
            u_all = jnp.where(sub == j, u[j], u_all)
            v_all = jnp.where(sub == j, v[j], v_all)
        t_ref[pl.ds(start, G), :] = v_all
        both = jnp.concatenate([u_all, v_all], axis=1)
        high = both.astype(BF16).astype(F32)
        low = both - high
        lhs = jnp.concatenate([high[:, :TILE], high[:, :TILE], low[:, :TILE], low[:, :TILE]], axis=0)
        rhs = jnp.concatenate([high, low, high, low], axis=0)
        d_ref[...] -= dot(lhs.astype(BF16), rhs.astype(BF16), ((0,), (0,)))
        return carry

    lax.fori_loop(0, TILE // G, step, 0)


def apply_kernel(bands, groups, m_ref, w, blk, ace, exch, a, rest, d_ref, t_ref, x16, proj,
                 bfull, applied, loc, b_s, b_r, p_s, p_r, e_s, e_r, *scratch):
    at = Place(bands, groups)
    me = at.me
    own, bown = ace.shape[0], exch.shape[0]
    cols = w.shape[1]
    n, nblk = own * bands, bown * bands
    scale = 1.0 / (ace.shape[1] * groups)
    greet(at.everyone())

    def chunk(index):
        return pl.ds(pl.multiple_of(index * cols, TILE), cols)

    mine = bfull.at[span(me, bown)]
    local = pltpu.make_async_copy(blk.at[:, chunk(me)], mine, loc.at[0])
    local.start()
    blocks = [send(blk.at[:, chunk(at.peer[d])], mine, b_s.at[d], b_r.at[d], at.band(d))
              for d in at.far]
    row = 0
    for s in range(0, n, TILE):
        for c in range(0, s + TILE, TILE):
            a[s:s + TILE, c:c + TILE] = m_ref[row:row + TILE, :].astype(F32) * -scale
            row += TILE
    rest[...] = identity(n)
    x16[...] = jnp.zeros_like(x16)
    p32, p16, allg = scratch[0], scratch[1], scratch[11]

    def stages():
        local.wait()
        for copy in blocks:
            copy.wait()
        half = nblk // 2
        for h in range(2):
            product = dot(w[...], bfull[h * half:(h + 1) * half, :], ((1,), (1,)))
            p32[h * n:(h + 1) * n, :] = product
            p16[h * n:(h + 1) * n, :] = product.astype(BF16)
        yield from reduce_stages(at, scratch)

    cuts = sorted(set(range(0, n, TILE)) | set(range(0, n, own)) | {n})
    pieces = list(enumerate(zip(cuts[:-1], cuts[1:])))

    def piece(q, r0, r1, source, target):
        lo = r0 % own
        return pltpu.make_async_remote_copy(
            src_ref=proj.at[r0:r1], dst_ref=ace.at[lo:lo + r1 - r0, chunk(source)],
            send_sem=p_s.at[q], recv_sem=p_r.at[q, source],
            device_id={"band": target}, device_id_type=MESH)

    def kept(q, r0, r1):
        lo = r0 % own
        return pltpu.make_async_copy(
            proj.at[r0:r1], ace.at[lo:lo + r1 - r0, chunk(me)], p_s.at[q])

    steps = stages()
    for s in range(0, n, TILE):
        e = s + TILE
        d_ref[:, 0:TILE] = a[s:e, s:e]
        d_ref[:, TILE:] = identity(TILE)
        factor_tile(d_ref, t_ref)
        tile = t_ref[...]
        rows = product3(tile, rest[s:e, 0:e], ((1,), (0,)))
        high, low = split(rows)
        x16[s:e, 0:e] = high
        proj[s:e, :] = (dot(high, w[0:e, :], ((1,), (0,)))
                        + dot(low, w[0:e, :], ((1,), (0,)))).astype(BF16)
        for q, (r0, r1) in pieces:
            if s <= r0 < e:
                owner = r0 // own

                @pl.when(me != owner)
                def _():
                    piece(q, r0, r1, me, owner).start()

                @pl.when(me == owner)
                def _():
                    kept(q, r0, r1).start()
        if e < n:
            panel = product3(a[e:, s:e], tile, ((1,), (1,)))
            for c in range(e, n, TILE):
                a[c:, c:c + TILE] -= product3(panel[c - e:], panel[c - e:c - s], ((1,), (1,)))
            rest[e:, 0:e] -= product3(panel, rows, ((1,), (0,)))
        next(steps, None)
    for _ in steps:
        pass
    half = nblk // 2
    for h in range(2):
        coupling = dot(x16[...], allg[h * n:(h + 1) * n, :], ((1,), (0,))) * scale
        applied[h * half:(h + 1) * half, :] = (
            -dot(coupling.astype(BF16), proj[...], ((0,), (0,)))).astype(BF16)
    outs = [send(applied.at[span(at.peer[d], bown)], exch.at[:, chunk(me)],
                 e_s.at[d], e_r.at[d], at.band(d)) for d in at.far]
    outs.append(pltpu.make_async_copy(applied.at[span(me, bown)], exch.at[:, chunk(me)], loc.at[1]))
    outs[-1].start()
    for q, (r0, r1) in pieces:
        owner = r0 // own

        @pl.when(me != owner)
        def _():
            piece(q, r0, r1, me, owner).wait_send()

        @pl.when(me == owner)
        def _():
            kept(q, r0, r1).wait()
            for d in range(1, bands):
                piece(q, r0, r1, at.peer[d], at.peer[d]).wait_recv()
    for copy in outs:
        copy.wait()


def shards(orbitals, kernel, block_vectors):
    groups, bands = lax.axis_size("ga"), lax.axis_size("band")
    own, width = orbitals.shape
    bown = block_vectors.shape[0]
    cols = width // bands
    n, nblk = own * bands, bown * bands
    levels = max(groups.bit_length() - 3, 1)
    unit = 4 * bands * 16
    tiles = n // TILE
    flat = -(-(tiles * (tiles + 1) // 2 * TILE) // unit) * unit
    pieces = len(set(range(0, n, TILE)) | set(range(0, n, own)))
    vmem, hbm = pl.BlockSpec(memory_space=pltpu.VMEM), pl.BlockSpec(memory_space=pl.ANY)
    dma = pltpu.SemaphoreType.DMA
    many = dma((bands,))
    margin, weighted = pl.pallas_call(
        functools.partial(margin_kernel, bands, groups),
        name="margin",
        out_shape=(
            jax.ShapeDtypeStruct((flat, TILE), BF16),
            jax.ShapeDtypeStruct((n, cols), BF16),
        ),
        in_specs=[hbm, vmem],
        out_specs=(vmem, vmem),
        scratch_shapes=[pltpu.VMEM((n, cols), BF16), dma((1,)), many, many]
        + reduce_scratch(flat, bands, levels),
        compiler_params=pltpu.CompilerParams(
            collective_id=0, has_side_effects=True, vmem_limit_bytes=48 * 2**20),
    )(orbitals, kernel.reshape(1, width))
    return pl.pallas_call(
        functools.partial(apply_kernel, bands, groups),
        name="apply",
        out_shape=(
            jax.ShapeDtypeStruct((own, width), BF16),
            jax.ShapeDtypeStruct((bown, width), BF16),
        ),
        in_specs=[vmem, vmem, hbm],
        out_specs=(hbm, hbm),
        scratch_shapes=[
            pltpu.VMEM((n, n), F32),
            pltpu.VMEM((n, n), F32),
            pltpu.VMEM((TILE, 2 * TILE), F32),
            pltpu.VMEM((TILE, TILE), F32),
            pltpu.VMEM((n, n), BF16),
            pltpu.VMEM((n, cols), BF16),
            pltpu.VMEM((nblk, cols), BF16),
            pltpu.VMEM((nblk, cols), BF16),
            dma((2,)), many, many, dma((pieces,)), dma((pieces, bands)), many, many,
        ] + reduce_scratch(2 * n, bands, levels),
        compiler_params=pltpu.CompilerParams(
            collective_id=1, has_side_effects=True, vmem_limit_bytes=48 * 2**20),
    )(margin, weighted, block_vectors)


def solution(mesh):
    placed = (P(("img", "band"), "ga"), P("ga"), P(("img", "band"), "ga"))
    return jax.shard_map(
        shards,
        mesh=mesh,
        in_specs=placed,
        out_specs=(P(("img", "band"), "ga"), P(("img", "band"), "ga")),
        check_vma=False,
    )
```

```python
import functools

import jax
import jax.numpy as jnp
from jax import lax
from jax.experimental import pallas as pl
from jax.experimental.pallas import tpu as pltpu
from jax.sharding import PartitionSpec as P

MESH = pl.DeviceIdType.MESH
F32 = jnp.float32
BF16 = jnp.bfloat16
TILE = 128


def send(src, dst, send_sem, recv_sem, where):
    copy = pltpu.make_async_remote_copy(
        src_ref=src, dst_ref=dst, send_sem=send_sem, recv_sem=recv_sem,
        device_id=where, device_id_type=MESH,
    )
    copy.start()
    return copy


def greet(places):
    barrier = pltpu.get_barrier_semaphore()
    for place in places:
        pl.semaphore_signal(barrier, inc=1, device_id=place, device_id_type=MESH)
    pl.semaphore_wait(barrier, len(places))


def dot(a, b, dims):
    return lax.dot_general(a, b, (dims, ((), ())), preferred_element_type=F32)


class Place:
    def __init__(self, bands, groups):
        self.bands = bands
        self.me = lax.axis_index("band")
        ga = lax.axis_index("ga")
        self.core = lax.rem(ga, 2)
        self.row = lax.rem(ga // 2, 2)
        self.partner = {"ga": ga + 1 - 2 * self.core}
        self.across = {"ga": ga + 2 - 4 * self.row}
        self.peer = [lax.rem(self.me + d, bands) for d in range(bands)]
        self.far = sorted(range(1, bands), key=lambda d: -min(d, bands - d))
        self.near = self.far[::-1]
        self.bits = []
        stride = 4
        while stride < groups:
            self.bits.append({"ga": ga + stride * (1 - 2 * lax.rem(ga // stride, 2))})
            stride *= 2

    def band(self, d):
        return {"band": self.peer[d]}

    def everyone(self):
        return [self.band(d) for d in range(1, self.bands)] + [self.partner, self.across] + self.bits


def span(index, size, offset=0):
    return pl.ds(pl.multiple_of(offset + index * size, 16), size)


def reduce_scratch(rows, bands, levels):
    h1, h2 = rows // 2, rows // 4
    h3 = h2 // bands
    dma = pltpu.SemaphoreType.DMA
    shapes = [
        ((rows, TILE), F32), ((rows, TILE), BF16), ((h1, TILE), BF16),
        ((h1, TILE), F32), ((h1, TILE), BF16), ((h2, TILE), BF16),
        ((h2, TILE), F32), ((h2, TILE), BF16), ((bands, h3, TILE), BF16),
        ((levels, h3, TILE), BF16), ((levels, h3, TILE), BF16), ((rows, TILE), BF16),
    ]
    return [pltpu.VMEM(*shape) for shape in shapes] + [
        dma((4,)), dma((bands,)), dma((bands,)), dma((levels,)), dma((levels,)),
        dma((bands,)), dma((bands,)), dma((bands,)), dma((bands,)),
        dma((2 * bands,)), dma((2 * bands,)),
    ]


def reduce_stages(at, scratch):
    (p32, p16, rx1, a32, a16, rx2, b32, b16, rx3, out_x, rx_x, allg,
     one, z_s, z_r, x_s, x_r, g_s, g_r, y_s, y_r, f_s, f_r) = scratch
    h1, h2 = rx1.shape[0], rx2.shape[0]
    h3 = h2 // at.bands
    copy = send(p16.at[span(1 - at.core, h1)], rx1, one.at[0], one.at[1], at.partner)
    yield
    copy.wait()
    a32[...] = p32[span(at.core, h1), :] + rx1[...].astype(F32)
    a16[...] = a32[...].astype(BF16)
    copy = send(a16.at[span(1 - at.row, h2)], rx2, one.at[2], one.at[3], at.across)
    yield
    copy.wait()
    b32[...] = a32[span(at.row, h2), :] + rx2[...].astype(F32)
    b16[...] = b32[...].astype(BF16)
    copies = [send(b16.at[span(at.peer[d], h3)], rx3.at[d], z_s.at[d], z_r.at[d], at.band(d))
              for d in at.far]
    yield
    for copy in copies:
        copy.wait()
    total = b32[span(at.me, h3), :]
    for d in range(1, at.bands):
        total = total + rx3[d].astype(F32)
    for i, place in enumerate(at.bits):
        out_x[i] = total.astype(BF16)
        send(out_x.at[i], rx_x.at[i], x_s.at[i], x_r.at[i], place).wait()
        total = out_x[i].astype(F32) + rx_x[i].astype(F32)

    def piece(d, row):
        source = lax.rem(at.me + at.bands - d, at.bands)
        return allg.at[span(source, h3, at.core * h1 + row * h2)]

    allg[span(at.me, h3, at.core * h1 + at.row * h2), :] = total.astype(BF16)
    own = piece(0, at.row)
    gathers = {d: send(own, own, g_s.at[d], g_r.at[d], at.band(d)) for d in at.far}
    sides = {0: send(own, own, y_s.at[0], y_r.at[0], at.across)}
    lasts = [send(own, own, f_s.at[0], f_r.at[0], at.partner)]
    yield
    for d in at.near:
        gathers[d].wait()
        there = piece(d, at.row)
        sides[d] = send(there, there, y_s.at[d], y_r.at[d], at.across)
        lasts.append(send(there, there, f_s.at[d], f_r.at[d], at.partner))
    yield
    for d in [0] + at.near:
        sides[d].wait()
        there = piece(d, 1 - at.row)
        e = at.bands + d
        lasts.append(send(there, there, f_s.at[e], f_r.at[e], at.partner))
    yield
    for copy in lasts:
        copy.wait()


def margin_kernel(bands, groups, orb, kern, m_out, w_out, full, loc, a_s, a_r, *scratch):
    at = Place(bands, groups)
    own = orb.shape[0]
    cols = orb.shape[1] // bands
    n = own * bands
    greet(at.everyone())

    def chunk(d):
        return pl.ds(pl.multiple_of(at.peer[d] * cols, TILE), cols)

    mine = full.at[span(at.me, own)]
    local = pltpu.make_async_copy(orb.at[:, chunk(0)], mine, loc.at[0])
    local.start()
    copies = [send(orb.at[:, chunk(d)], mine, a_s.at[d], a_r.at[d], at.band(d)) for d in at.far]
    local.wait()
    for copy in copies:
        copy.wait()
    w_out[...] = (-(full[...].astype(F32) * kern[:, chunk(0)])).astype(BF16)
    p32, p16, allg = scratch[0], scratch[1], scratch[11]
    row = 0
    for s in range(0, n, TILE):
        e = s + TILE
        product = dot(w_out[s:e, :], full[0:e, :], ((1,), (1,)))
        for c in range(0, e, TILE):
            p32[row:row + TILE, :] = product[:, c:c + TILE]
            p16[row:row + TILE, :] = product[:, c:c + TILE].astype(BF16)
            row += TILE
    if row < p32.shape[0]:
        p32[row:, :] = jnp.zeros((p32.shape[0] - row, TILE), F32)
        p16[row:, :] = jnp.zeros((p32.shape[0] - row, TILE), BF16)
    for _ in reduce_stages(at, scratch):
        pass
    m_out[...] = allg[...]


def split(a):
    high = a.astype(BF16)
    return high, (a - high.astype(F32)).astype(BF16)


def product3(a, b, dims):
    (ah, al), (bh, bl) = split(a), split(b)
    return dot(ah, bh, dims) + (dot(ah, bl, dims) + dot(al, bh, dims))


def identity(rows):
    shape = (rows, rows)
    return (lax.broadcasted_iota(jnp.int32, shape, 0)
            == lax.broadcasted_iota(jnp.int32, shape, 1)).astype(F32)


def factor_tile(d_ref, t_ref):
    G, SUB = 32, 8
    H = G // SUB
    sub = lax.broadcasted_iota(jnp.int32, (SUB, TILE), 0)

    def spread(block, i):
        return jnp.broadcast_to(block[i:i + 1, :], (SUB, TILE))

    def lane(block, c):
        return jnp.broadcast_to(block[:, c:c + 1], (SUB, TILE))

    def step(g, carry):
        start = pl.multiple_of(g * G, G)
        turned = pltpu.roll(d_ref[pl.ds(start, G), 0:TILE], lax.rem(TILE - start, TILE), 1)
        right = d_ref[pl.ds(start, G), TILE:2 * TILE]
        lefts = [turned[h * SUB:(h + 1) * SUB, :] for h in range(H)]
        rights = [right[h * SUB:(h + 1) * SUB, :] for h in range(H)]
        us, vs = [], []
        for b in range(H):
            columns = [lane(lefts[b], b * SUB + c) for c in range(SUB)]
            d = [[spread(columns[c], i) for c in range(i + 1)] for i in range(SUB)]
            below = {h: [lane(lefts[h], b * SUB + c) for c in range(SUB)] for h in range(b + 1, H)}
            u, v = [], []
            u_all = v_all = jnp.zeros((SUB, TILE), F32)
            for j in range(SUB):
                r = lax.rsqrt(d[j][j])
                for i in range(j + 1, SUB):
                    d[i][j] = d[i][j] * r
                for i in range(j + 1, SUB):
                    for c in range(j + 1, i + 1):
                        d[i][c] = d[i][c] - d[i][j] * d[c][j]
                p, q = spread(lefts[b], j), spread(rights[b], j)
                for t in range(j):
                    p = p - d[j][t] * u[t]
                    q = q - d[j][t] * v[t]
                u.append(p * r)
                v.append(q * r)
                u_all = jnp.where(sub == j, u[j], u_all)
                v_all = jnp.where(sub == j, v[j], v_all)
                for h in range(b + 1, H):
                    n = below[h][j]
                    for t in range(j):
                        n = n - below[h][t] * d[j][t]
                    below[h][j] = n * r
            us.append(u_all)
            vs.append(v_all)
            for h in range(b + 1, H):
                for j in range(SUB):
                    lefts[h] = lefts[h] - below[h][j] * u[j]
                    rights[h] = rights[h] - below[h][j] * v[j]
        u_all = pltpu.roll(jnp.concatenate(us, axis=0), start, 1)
        v_all = jnp.concatenate(vs, axis=0)
        t_ref[pl.ds(start, G), :] = v_all
        both = jnp.concatenate([u_all, v_all], axis=1)
        high = both.astype(BF16).astype(F32)
        low = both - high
        lhs = jnp.concatenate([high[:, :TILE], high[:, :TILE], low[:, :TILE]], axis=0)
        rhs = jnp.concatenate([high, low, high], axis=0)
        d_ref[...] -= dot(lhs.astype(BF16), rhs.astype(BF16), ((0,), (0,)))
        return carry

    lax.fori_loop(0, TILE // G, step, 0)


def apply_kernel(bands, groups, m_ref, w, blk, ace, exch, a, rest, d_ref, t_ref, x16, proj,
                 bfull, applied, loc, b_s, b_r, p_s, p_r, e_s, e_r, *scratch):
    at = Place(bands, groups)
    me = at.me
    own, bown = ace.shape[0], exch.shape[0]
    cols = w.shape[1]
    n, nblk = own * bands, bown * bands
    scale = 1.0 / (ace.shape[1] * groups)
    greet(at.everyone())

    def chunk(index):
        return pl.ds(pl.multiple_of(index * cols, TILE), cols)

    mine = bfull.at[span(me, bown)]
    local = pltpu.make_async_copy(blk.at[:, chunk(me)], mine, loc.at[0])
    local.start()
    blocks = [send(blk.at[:, chunk(at.peer[d])], mine, b_s.at[d], b_r.at[d], at.band(d))
              for d in at.far]
    row = 0
    for s in range(0, n, TILE):
        for c in range(0, s + TILE, TILE):
            a[s:s + TILE, c:c + TILE] = m_ref[row:row + TILE, :].astype(F32) * -scale
            row += TILE
    rest[...] = identity(n)
    x16[...] = jnp.zeros_like(x16)
    p32, p16, allg = scratch[0], scratch[1], scratch[11]

    def stages():
        local.wait()
        for copy in blocks:
            copy.wait()
        half = nblk // 2
        for h in range(2):
            product = dot(w[...], bfull[h * half:(h + 1) * half, :], ((1,), (1,)))
            p32[h * n:(h + 1) * n, :] = product
            p16[h * n:(h + 1) * n, :] = product.astype(BF16)
        yield from reduce_stages(at, scratch)

    cuts = sorted(set(range(0, n, TILE)) | set(range(0, n, own)) | {n})
    pieces = list(enumerate(zip(cuts[:-1], cuts[1:])))

    def piece(q, r0, r1, source, target):
        lo = r0 % own
        return pltpu.make_async_remote_copy(
            src_ref=proj.at[r0:r1], dst_ref=ace.at[lo:lo + r1 - r0, chunk(source)],
            send_sem=p_s.at[q], recv_sem=p_r.at[q, source],
            device_id={"band": target}, device_id_type=MESH)

    def kept(q, r0, r1):
        lo = r0 % own
        return pltpu.make_async_copy(
            proj.at[r0:r1], ace.at[lo:lo + r1 - r0, chunk(me)], p_s.at[q])

    steps = stages()
    for s in range(0, n, TILE):
        e = s + TILE
        d_ref[:, 0:TILE] = a[s:e, s:e]
        d_ref[:, TILE:] = identity(TILE)
        factor_tile(d_ref, t_ref)
        tile = t_ref[...]
        rows = product3(tile, rest[s:e, 0:e], ((1,), (0,)))
        high, low = split(rows)
        x16[s:e, 0:e] = high
        proj[s:e, :] = (dot(high, w[0:e, :], ((1,), (0,)))
                        + dot(low, w[0:e, :], ((1,), (0,)))).astype(BF16)
        for q, (r0, r1) in pieces:
            if s <= r0 < e:
                owner = r0 // own

                @pl.when(me != owner)
                def _():
                    piece(q, r0, r1, me, owner).start()

                @pl.when(me == owner)
                def _():
                    kept(q, r0, r1).start()
        if e < n:
            panel = product3(a[e:, s:e], tile, ((1,), (1,)))
            for c in range(e, n, TILE):
                a[c:, c:c + TILE] -= product3(panel[c - e:], panel[c - e:c - s], ((1,), (1,)))
            rest[e:, 0:e] -= product3(panel, rows, ((1,), (0,)))
        next(steps, None)
    for _ in steps:
        pass
    half = nblk // 2
    for h in range(2):
        coupling = dot(x16[...], allg[h * n:(h + 1) * n, :], ((1,), (0,))) * scale
        applied[h * half:(h + 1) * half, :] = (
            -dot(coupling.astype(BF16), proj[...], ((0,), (0,)))).astype(BF16)
    outs = [send(applied.at[span(at.peer[d], bown)], exch.at[:, chunk(me)],
                 e_s.at[d], e_r.at[d], at.band(d)) for d in at.far]
    outs.append(pltpu.make_async_copy(applied.at[span(me, bown)], exch.at[:, chunk(me)], loc.at[1]))
    outs[-1].start()
    for q, (r0, r1) in pieces:
        owner = r0 // own

        @pl.when(me != owner)
        def _():
            piece(q, r0, r1, me, owner).wait_send()

        @pl.when(me == owner)
        def _():
            kept(q, r0, r1).wait()
            for d in range(1, bands):
                piece(q, r0, r1, at.peer[d], at.peer[d]).wait_recv()
    for copy in outs:
        copy.wait()


def shards(orbitals, kernel, block_vectors):
    groups, bands = lax.axis_size("ga"), lax.axis_size("band")
    own, width = orbitals.shape
    bown = block_vectors.shape[0]
    cols = width // bands
    n, nblk = own * bands, bown * bands
    levels = max(groups.bit_length() - 3, 1)
    unit = 4 * bands * 16
    tiles = n // TILE
    flat = -(-(tiles * (tiles + 1) // 2 * TILE) // unit) * unit
    pieces = len(set(range(0, n, TILE)) | set(range(0, n, own)))
    vmem, hbm = pl.BlockSpec(memory_space=pltpu.VMEM), pl.BlockSpec(memory_space=pl.ANY)
    dma = pltpu.SemaphoreType.DMA
    many = dma((bands,))
    margin, weighted = pl.pallas_call(
        functools.partial(margin_kernel, bands, groups),
        name="margin",
        out_shape=(
            jax.ShapeDtypeStruct((flat, TILE), BF16),
            jax.ShapeDtypeStruct((n, cols), BF16),
        ),
        in_specs=[hbm, vmem],
        out_specs=(vmem, vmem),
        scratch_shapes=[pltpu.VMEM((n, cols), BF16), dma((1,)), many, many]
        + reduce_scratch(flat, bands, levels),
        compiler_params=pltpu.CompilerParams(
            collective_id=0, has_side_effects=True, vmem_limit_bytes=48 * 2**20),
    )(orbitals, kernel.reshape(1, width))
    return pl.pallas_call(
        functools.partial(apply_kernel, bands, groups),
        name="apply",
        out_shape=(
            jax.ShapeDtypeStruct((own, width), BF16),
            jax.ShapeDtypeStruct((bown, width), BF16),
        ),
        in_specs=[vmem, vmem, hbm],
        out_specs=(hbm, hbm),
        scratch_shapes=[
            pltpu.VMEM((n, n), F32),
            pltpu.VMEM((n, n), F32),
            pltpu.VMEM((TILE, 2 * TILE), F32),
            pltpu.VMEM((TILE, TILE), F32),
            pltpu.VMEM((n, n), BF16),
            pltpu.VMEM((n, cols), BF16),
            pltpu.VMEM((nblk, cols), BF16),
            pltpu.VMEM((nblk, cols), BF16),
            dma((2,)), many, many, dma((pieces,)), dma((pieces, bands)), many, many,
        ] + reduce_scratch(2 * n, bands, levels),
        compiler_params=pltpu.CompilerParams(
            collective_id=1, has_side_effects=True, vmem_limit_bytes=48 * 2**20),
    )(margin, weighted, block_vectors)


def solution(mesh):
    placed = (P(("img", "band"), "ga"), P("ga"), P(("img", "band"), "ga"))
    return jax.shard_map(
        shards,
        mesh=mesh,
        in_specs=placed,
        out_specs=(P(("img", "band"), "ga"), P(("img", "band"), "ga")),
        check_vma=False,
    )
```
